32 devices in a mesh: wide: 8 (over y, x, core), narrow: 4 (over z).
Axes of the slice: x: 2, y: 2, z: 4, core: 2. Of those that a mesh axis runs over, the one named last changes fastest.
Arguments:
- image: bfloat16 [2, 256, 256, 256], P(None, 'wide', 'narrow'), may hold values from -6 to 6
- deapodization: float32 [3, 256], replicated, may hold values from 0.5 to 2
- offsets: int32 [32, 8], P(('wide', 'narrow')), may hold values from 0 to 256
- cross_weight: bfloat16 [32, 8, 1536, 1024], P(('wide', 'narrow')), may hold values from -0.1875 to 0.1875
- x_weight: bfloat16 [32, 8, 1536, 256], P(('wide', 'narrow')), may hold values from -0.375 to 0.375
Outputs:
- samples: float32 [32, 8, 2, 1536], P(('wide', 'narrow'))
The draws below stay inside these ranges and needn't reach their ends.
Inputs may be any that keep to these rules, and one draw needn't show every extreme that they name: `offsets`: each entry is the first row, along the first frequency dimension, of a group's window of 256 rows in one slab.
All inputs are finite; a program needn't handle non-finite values.
Results may differ from the reference program's by a relative error of at most 0.007.
Values may be sent and summed in bfloat16 or wider, within the bound.
A program may use at most 128 MiB of HBM per device.

```python
import math
import jax
import jax.numpy as jnp
from jax import lax

N = 256
G = 512
KZ = 64
BX = 256
SAMP = 1536
CROSS = 1024
GROUPS = 32
N_WIDE = 8
N_NARROW = 4


def plant(array, stream_key, least, high):
    place = [jax.random.randint(jax.random.fold_in(stream_key, axis), (), 0, length) for axis, length in enumerate(array.shape)]
    longest = array.shape.index(max(array.shape))
    beside = place[:longest] + [(place[longest] + 1) % array.shape[longest]] + place[longest + 1:]
    return array.at[tuple(place)].set(least).at[tuple(beside)].set(high)


def steps_of(key, shape, cuts, least, high):
    level = 1.0
    for axis_at, shards_of in cuts:
        heights = jax.random.uniform(jax.random.fold_in(jax.random.fold_in(key, 6), axis_at), (shards_of,), jnp.float32, least / len(cuts), high / len(cuts))
        level = level * jnp.repeat(jnp.exp(heights), shape[axis_at] // shards_of).reshape((-1,) + (1,) * (len(shape) - 1 - axis_at))
    return level


def normal_values(key, dims, width, most, split=(), held_as=jnp.bfloat16):
    result = jax.random.normal(key, dims, jnp.float32) * width
    if len(split) > 0:
        result = steps_of(key, dims, split, -0.22, 0.18) * result
    return jnp.clip(result, min=-most, max=most).astype(held_as)


def setup_inputs(seed: int = 0) -> dict:
    arg_keys = jax.random.split(jax.random.key(seed), 6)
    return {
        "image": normal_values(arg_keys[0], (2, N, N, N), 1.0, 6.0, ((1, 8), (2, 4))),
        "deapodization": jnp.clip(jnp.exp(jax.random.uniform(arg_keys[1], (3, N), jnp.float32, math.log(0.5), math.log(2.0))), 0.5, 2.0),
        "offsets": plant(jax.random.randint(arg_keys[2], (GROUPS, N_WIDE), 0, G - BX + 1), jax.random.fold_in(arg_keys[2], 1), 0, G - BX).astype(jnp.int32),
        "cross_weight": normal_values(arg_keys[3], (GROUPS, N_WIDE, SAMP, CROSS), CROSS ** -0.5, 0.1875, ((0, 32),)),
        "x_weight": normal_values(arg_keys[4], (GROUPS, N_WIDE, SAMP, BX), BX ** -0.5, 0.375, ((0, 32),)),
    }


def dft_tables(out_rows, inputs, grid_size, lowest):
    frequency = jnp.arange(out_rows, dtype=jnp.int32) + lowest
    position = jnp.arange(inputs, dtype=jnp.int32) - inputs // 2
    phases = jnp.mod(frequency[:, None] * position[None, :], grid_size)
    angles = phases.astype(jnp.float32) * (2.0 * math.pi / grid_size)
    factor = 1.0 / math.sqrt(inputs)
    return jnp.stack([jnp.cos(angles) * factor, jnp.sin(angles) * factor]).astype(jnp.bfloat16)

def mix_parts(product):
    return (product[0, 0] + product[1, 1], product[0, 1] - product[1, 0])

def reference(image, deapodization, offsets, cross_weight, x_weight):
    weighted = (image.astype(jnp.float32) * deapodization[0][None, :, None, None] * deapodization[1][None, None, :, None] * deapodization[2][None, None, None, :]).astype(jnp.bfloat16)
    z_table = dft_tables(KZ, N, G, -(KZ // 2)).astype(jnp.float32)
    product = jnp.einsum('tkz,cxyz->tcxyk', z_table, weighted.astype(jnp.float32))
    real_part, imag_part = mix_parts(product)
    band_data = jnp.stack([real_part, imag_part], axis=0).astype(jnp.bfloat16)
    line_table = dft_tables(G, N, G, -(G // 2)).astype(jnp.float32)
    product = jnp.einsum('tqy,cxyk->tcxqk', line_table, band_data.astype(jnp.float32))
    real_part, imag_part = mix_parts(product)
    columns = jnp.stack([real_part, imag_part], axis=0).astype(jnp.bfloat16)
    product = jnp.einsum('tpx,cxqk->tcpqk', line_table, columns.astype(jnp.float32))
    real_part, imag_part = mix_parts(product)
    kspace = jnp.stack([real_part, imag_part], axis=1).astype(jnp.bfloat16)
    span_y = G // N_WIDE
    span_z = KZ // N_NARROW

    def group_samples(group_index):
        narrow_pos = group_index % N_NARROW

        def slab_samples(slab_index):
            start_row = offsets[group_index, slab_index]
            window_rows = lax.dynamic_slice(kspace, (start_row, jnp.int32(0), slab_index * span_y, narrow_pos * span_z), (BX, 2, span_y, span_z)).reshape(BX, 2, span_y * span_z)
            cross_rows = cross_weight[group_index, slab_index].astype(jnp.float32)
            partial_value = jnp.einsum('ms,qcs->cmq', cross_rows, window_rows.astype(jnp.float32))
            window_gain = x_weight[group_index, slab_index].astype(jnp.float32)
            return lax.optimization_barrier(jnp.sum(partial_value * window_gain[None], axis=-1))
        return lax.map(slab_samples, jnp.arange(N_WIDE, dtype=jnp.int32))
    return lax.map(group_samples, jnp.arange(N_WIDE * N_NARROW, dtype=jnp.int32))
```

```python
import functools
import math

import jax
import jax.numpy as jnp
import numpy as np
from jax import lax
from jax.experimental import pallas as pl
from jax.experimental.pallas import tpu as pltpu
from jax.sharding import PartitionSpec as P

G = 512
KZ = 64
BX = 256


def base_tables(out_rows, inputs, grid_size, lowest):
    frequency = np.arange(out_rows, dtype=np.int64) + lowest
    position = np.arange(inputs, dtype=np.int64) - inputs // 2
    phases = np.mod(frequency[:, None] * position[None, :], grid_size)
    angles = phases.astype(np.float64) * (2.0 * math.pi / grid_size)
    factor = 1.0 / math.sqrt(inputs)
    cosine = (np.cos(angles) * factor).astype(np.float32).astype(jnp.bfloat16)
    sine = (np.sin(angles) * factor).astype(np.float32).astype(jnp.bfloat16)
    return cosine, sine


def complex_table(cosine, sine):
    real_rows = np.stack([cosine, sine], axis=1)
    imag_rows = np.stack([-sine, cosine], axis=1)
    return np.stack([real_rows, imag_rows], axis=0)


def sample_kernel(
    sizes, offsets_ref, band_ref, line_ref, row_ref, x_ref, cross_ref, out_ref, wide_ref, slab_ref, window_ref
):
    depth, grid_rows, width, tile = sizes
    step = pl.program_id(0)
    cells = slab_ref.shape[0]

    @pl.when(step == 0)
    def _():
        def one_plane(k, carry):
            parts = [
                band_ref[:, piece, k].reshape(width, band_ref.shape[-1])
                for piece in range(band_ref.shape[1])
            ]
            plane = jnp.concatenate(parts, axis=-1) if len(parts) > 1 else parts[0]
            lines = lax.dot_general(
                line_ref[...], plane, (((1,), (1,)), ((), ())), preferred_element_type=jnp.float32
            )
            for part in range(2):
                for lane in range(0, width, 128):
                    wide_ref[(part * width + lane) // 128, pl.ds(k, grid_rows, stride=depth), :] = lines[
                        part * grid_rows : (part + 1) * grid_rows, lane : lane + 128
                    ]
            return carry

        for k in range(depth):
            one_plane(k, 0)

    here = pl.ds(pl.multiple_of(step * cells, cells), cells)
    start = offsets_ref[0, step]
    for block in range(2 * width // 128):
        lanes = slice(block * 128, (block + 1) * 128)
        slab_ref[:, lanes] = wide_ref[block, here, :].astype(jnp.bfloat16)
        window_ref[:, lanes] = row_ref[block, pl.ds(start, BX), :].astype(jnp.bfloat16)
    for first in range(0, cross_ref.shape[1], tile):
        rows = slice(first, first + tile)
        partial = jnp.dot(cross_ref[0, rows], slab_ref[...], preferred_element_type=jnp.float32)
        gain = jnp.dot(x_ref[0, rows], window_ref[...], preferred_element_type=jnp.float32)
        part_re, part_im = partial[:, :width], partial[:, width:]
        gain_cos, gain_sin = gain[:, :width], gain[:, width:]
        for part, value in enumerate(
            (gain_cos * part_re + gain_sin * part_im, gain_cos * part_im - gain_sin * part_re)
        ):
            folded = value[:, :128]
            for lane in range(128, width, 128):
                folded = folded + value[:, lane : lane + 128]
            out_ref[0, part : part + 1, rows] = jnp.sum(folded.T, axis=0, keepdims=True)


def per_device(image, deapodization, offsets, cross_weight, x_weight):
    wide_count = lax.axis_size("wide")
    narrow_count = lax.axis_size("narrow")
    wide_index = lax.axis_index("wide")
    narrow_index = lax.axis_index("narrow")
    block_x = image.shape[1]
    block_y = image.shape[2]
    width = image.shape[3]
    depth = KZ // narrow_count
    samples, cells = cross_weight.shape[2], cross_weight.shape[3]
    scale_x = lax.dynamic_slice_in_dim(deapodization[0], wide_index * block_x, block_x)
    scale_y = lax.dynamic_slice_in_dim(deapodization[1], narrow_index * block_y, block_y)
    weighted = (
        image.astype(jnp.float32)
        * scale_x[None, :, None, None]
        * scale_y[None, None, :, None]
        * deapodization[2][None, None, None, :]
    ).astype(jnp.bfloat16)
    z_table = complex_table(*base_tables(KZ, width, G, -(KZ // 2)))
    band = jnp.einsum(
        "okcz,cxyz->kxoy", jnp.asarray(z_table), weighted, preferred_element_type=jnp.float32
    ).astype(jnp.bfloat16)
    band = band.reshape(KZ, block_x, 2 * block_y)
    band = lax.all_to_all(band, "narrow", split_axis=0, concat_axis=0, tiled=True)
    band = lax.all_gather(band, "wide", axis=0, tiled=False)
    band = band.reshape(wide_count, narrow_count, depth, block_x, 2 * block_y)
    if (2 * block_y) % 128:
        band = band.transpose(0, 2, 3, 1, 4).reshape(wide_count, 1, depth, block_x, 2 * width)

    cosine, sine = base_tables(G, width, G, -(G // 2))
    line_table = complex_table(cosine, sine).reshape(2 * G, 2, narrow_count, block_y)
    line_table = line_table.transpose(0, 2, 1, 3).reshape(2 * G, 2 * width)
    row_table = np.concatenate([cosine, sine], axis=1).astype(np.float32)
    row_table = row_table.reshape(G, 2 * width // 128, 128).transpose(1, 0, 2)

    tile = 512 if samples % 512 == 0 else samples
    kernel = functools.partial(sample_kernel, (depth, G, width, tile))
    out = pl.pallas_call(
        kernel,
        grid=(wide_count,),
        out_shape=jax.ShapeDtypeStruct((wide_count, 2, samples), jnp.float32),
        in_specs=[
            pl.BlockSpec(memory_space=pltpu.SMEM),
            pl.BlockSpec(band.shape, lambda s: (0, 0, 0, 0, 0)),
            pl.BlockSpec(line_table.shape, lambda s: (0, 0)),
            pl.BlockSpec(row_table.shape, lambda s: (0, 0, 0)),
            pl.BlockSpec((1, samples, BX), lambda s: (s, 0, 0)),
            pl.BlockSpec((1, samples, cells), lambda s: (s, 0, 0)),
        ],
        out_specs=pl.BlockSpec((1, 2, samples), lambda s: (s, 0, 0)),
        scratch_shapes=[
            pltpu.VMEM((2 * width // 128, G * depth, 128), jnp.float32),
            pltpu.VMEM((cells, 2 * width), jnp.bfloat16),
            pltpu.VMEM((BX, 2 * width), jnp.bfloat16),
        ],
        compiler_params=pltpu.CompilerParams(vmem_limit_bytes=60 * 1024 * 1024),
        cost_estimate=pl.CostEstimate(
            flops=2 * wide_count * samples * 2 * width * (cells + BX) + 8 * G * width * width * depth,
            bytes_accessed=2 * wide_count * samples * (cells + BX),
            transcendentals=0,
        ),
    )(offsets, band, jnp.asarray(line_table), jnp.asarray(row_table), x_weight[0], cross_weight[0])
    return out[None]


def solution(mesh):
    return jax.shard_map(
        per_device,
        mesh=mesh,
        in_specs=(
            P(None, "wide", "narrow", None),
            P(),
            P(("wide", "narrow"), None),
            P(("wide", "narrow"), None, None, None),
            P(("wide", "narrow"), None, None, None),
        ),
        out_specs=P(("wide", "narrow"), None, None, None),
        check_vma=False,
    )
```

```python
import functools
import math

import jax
import jax.numpy as jnp
import numpy as np
from jax import lax
from jax.experimental import pallas as pl
from jax.experimental.pallas import tpu as pltpu
from jax.sharding import PartitionSpec as P

G = 512
KZ = 64
BX = 256


def base_tables(out_rows, inputs, grid_size, lowest):
    frequency = np.arange(out_rows, dtype=np.int64) + lowest
    position = np.arange(inputs, dtype=np.int64) - inputs // 2
    phases = np.mod(frequency[:, None] * position[None, :], grid_size)
    angles = phases.astype(np.float64) * (2.0 * math.pi / grid_size)
    factor = 1.0 / math.sqrt(inputs)
    cosine = (np.cos(angles) * factor).astype(np.float32).astype(jnp.bfloat16)
    sine = (np.sin(angles) * factor).astype(np.float32).astype(jnp.bfloat16)
    return cosine, sine


def complex_table(cosine, sine):
    real_rows = np.stack([cosine, sine], axis=1)
    imag_rows = np.stack([-sine, cosine], axis=1)
    return np.stack([real_rows, imag_rows], axis=0)


def sample_kernel(
    sizes, offsets_ref, band_ref, line_ref, row_ref, x_ref, cross_ref, out_ref, wide_ref, slab_ref, window_ref
):
    depth, grid_rows, width, tile = sizes
    step = pl.program_id(0)
    cells = slab_ref.shape[0]

    @pl.when(step == 0)
    def _():
        def one_plane(k, carry):
            parts = [
                band_ref[:, piece, k].reshape(width, band_ref.shape[-1])
                for piece in range(band_ref.shape[1])
            ]
            plane = jnp.concatenate(parts, axis=-1) if len(parts) > 1 else parts[0]
            lines = lax.dot_general(
                line_ref[...], plane, (((1,), (1,)), ((), ())), preferred_element_type=jnp.float32
            )
            for part in range(2):
                for lane in range(0, width, 128):
                    wide_ref[(part * width + lane) // 128, pl.ds(k, grid_rows, stride=depth), :] = lines[
                        part * grid_rows : (part + 1) * grid_rows, lane : lane + 128
                    ]
            return carry

        for k in range(depth):
            one_plane(k, 0)

    here = pl.ds(pl.multiple_of(step * cells, cells), cells)
    start = offsets_ref[0, step]
    for block in range(2 * width // 128):
        lanes = slice(block * 128, (block + 1) * 128)
        slab_ref[:, lanes] = wide_ref[block, here, :].astype(jnp.bfloat16)
        window_ref[:, lanes] = row_ref[block, pl.ds(start, BX), :].astype(jnp.bfloat16)
    for first in range(0, cross_ref.shape[1], tile):
        rows = slice(first, first + tile)
        partial = jnp.dot(cross_ref[0, rows], slab_ref[...], preferred_element_type=jnp.float32)
        gain = jnp.dot(x_ref[0, rows], window_ref[...], preferred_element_type=jnp.float32)
        part_re, part_im = partial[:, :width], partial[:, width:]
        gain_cos, gain_sin = gain[:, :width], gain[:, width:]
        for part, value in enumerate(
            (gain_cos * part_re + gain_sin * part_im, gain_cos * part_im - gain_sin * part_re)
        ):
            folded = value[:, :128]
            for lane in range(128, width, 128):
                folded = folded + value[:, lane : lane + 128]
            out_ref[0, part : part + 1, rows] = jnp.sum(folded.T, axis=0, keepdims=True)


def gather_kernel(
    wide, narrow, band_ref, out_ref, own_sem, swap_send, swap_recv, chip_send, chip_recv, core_send, core_recv
):
    w = lax.axis_index("wide")
    n = lax.axis_index("narrow")
    sibling = w + 1 - 2 * lax.rem(w, 2)
    chips = wide // 2
    barrier = pltpu.get_barrier_semaphore()
    targets = [(w, lax.rem(n + j, narrow)) for j in range(1, narrow)]
    targets += [(lax.rem(w + 2 * j, wide), n) for j in range(1, chips)] + [(sibling, n)]
    for target in targets:
        pl.semaphore_signal(
            barrier, inc=1, device_id=target, device_id_type=pl.DeviceIdType.MESH
        )
    pl.semaphore_wait(barrier, len(targets))

    def remote(source, place, send, receive, target):
        return pltpu.make_async_remote_copy(
            src_ref=source,
            dst_ref=place,
            send_sem=send,
            recv_sem=receive,
            device_id=target,
            device_id_type=pl.DeviceIdType.MESH,
        )

    swaps = []
    for j in range(1, narrow):
        peer = lax.rem(n + j, narrow)
        swap = remote(
            band_ref.at[peer], out_ref.at[w, n], swap_send.at[j - 1], swap_recv.at[j - 1], (w, peer)
        )
        swap.start()
        swaps.append(swap)
    own = pltpu.make_async_copy(band_ref.at[n], out_ref.at[w, n], own_sem)
    own.start()
    own.wait()
    for swap in swaps:
        swap.wait()
    mine = out_ref.at[w]
    hops = []
    for j in range(1, chips):
        peer = lax.rem(w + 2 * j, wide)
        hop = remote(mine, mine, chip_send.at[j - 1], chip_recv.at[j - 1], (peer, n))
        hop.start()
        hops.append(hop)
    passes = [remote(mine, mine, core_send.at[0], core_recv.at[0], (sibling, n))]
    passes[0].start()
    for j in range(1, chips):
        hops[j - 1].wait_recv()
        block = out_ref.at[lax.rem(w + wide - 2 * j, wide)]
        forward = remote(block, block, core_send.at[j], core_recv.at[j], (sibling, n))
        forward.start()
        passes.append(forward)
    for hop in hops:
        hop.wait_send()
    for forward in passes:
        forward.wait()


def per_device(image, deapodization, offsets, cross_weight, x_weight):
    wide_count = lax.axis_size("wide")
    narrow_count = lax.axis_size("narrow")
    wide_index = lax.axis_index("wide")
    narrow_index = lax.axis_index("narrow")
    block_x = image.shape[1]
    block_y = image.shape[2]
    width = image.shape[3]
    depth = KZ // narrow_count
    samples, cells = cross_weight.shape[2], cross_weight.shape[3]
    scale_x = lax.dynamic_slice_in_dim(deapodization[0], wide_index * block_x, block_x)
    scale_y = lax.dynamic_slice_in_dim(deapodization[1], narrow_index * block_y, block_y)
    weighted = (
        image.astype(jnp.float32)
        * scale_x[None, :, None, None]
        * scale_y[None, None, :, None]
        * deapodization[2][None, None, None, :]
    ).astype(jnp.bfloat16)
    z_table = complex_table(*base_tables(KZ, width, G, -(KZ // 2)))
    band = jnp.einsum(
        "okcz,cxyz->kxoy", jnp.asarray(z_table), weighted, preferred_element_type=jnp.float32
    ).astype(jnp.bfloat16)
    band = band.reshape(KZ, block_x, 2 * block_y)
    band = band.reshape(narrow_count, depth, block_x, 2 * block_y)
    chips = wide_count // 2
    band = pl.pallas_call(
        functools.partial(gather_kernel, wide_count, narrow_count),
        out_shape=jax.ShapeDtypeStruct((wide_count,) + band.shape, band.dtype),
        in_specs=[pl.BlockSpec(memory_space=pltpu.VMEM)],
        out_specs=pl.BlockSpec(memory_space=pltpu.VMEM),
        scratch_shapes=[
            pltpu.SemaphoreType.DMA,
            pltpu.SemaphoreType.DMA((narrow_count - 1,)),
            pltpu.SemaphoreType.DMA((narrow_count - 1,)),
            pltpu.SemaphoreType.DMA((chips - 1,)),
            pltpu.SemaphoreType.DMA((chips - 1,)),
            pltpu.SemaphoreType.DMA((chips,)),
            pltpu.SemaphoreType.DMA((chips,)),
        ],
        compiler_params=pltpu.CompilerParams(collective_id=0, has_side_effects=True),
    )(band)
    if (2 * block_y) % 128:
        band = band.transpose(0, 2, 3, 1, 4).reshape(wide_count, 1, depth, block_x, 2 * width)

    cosine, sine = base_tables(G, width, G, -(G // 2))
    line_table = complex_table(cosine, sine).reshape(2 * G, 2, narrow_count, block_y)
    line_table = line_table.transpose(0, 2, 1, 3).reshape(2 * G, 2 * width)
    row_table = np.concatenate([cosine, sine], axis=1).astype(np.float32)
    row_table = row_table.reshape(G, 2 * width // 128, 128).transpose(1, 0, 2)

    tile = 512 if samples % 512 == 0 else samples
    kernel = functools.partial(sample_kernel, (depth, G, width, tile))
    out = pl.pallas_call(
        kernel,
        grid=(wide_count,),
        out_shape=jax.ShapeDtypeStruct((wide_count, 2, samples), jnp.float32),
        in_specs=[
            pl.BlockSpec(memory_space=pltpu.SMEM),
            pl.BlockSpec(band.shape, lambda s: (0, 0, 0, 0, 0)),
            pl.BlockSpec(line_table.shape, lambda s: (0, 0)),
            pl.BlockSpec(row_table.shape, lambda s: (0, 0, 0)),
            pl.BlockSpec((1, samples, BX), lambda s: (s, 0, 0)),
            pl.BlockSpec((1, samples, cells), lambda s: (s, 0, 0)),
        ],
        out_specs=pl.BlockSpec((1, 2, samples), lambda s: (s, 0, 0)),
        scratch_shapes=[
            pltpu.VMEM((2 * width // 128, G * depth, 128), jnp.float32),
            pltpu.VMEM((cells, 2 * width), jnp.bfloat16),
            pltpu.VMEM((BX, 2 * width), jnp.bfloat16),
        ],
        compiler_params=pltpu.CompilerParams(vmem_limit_bytes=60 * 1024 * 1024),
        cost_estimate=pl.CostEstimate(
            flops=2 * wide_count * samples * 2 * width * (cells + BX) + 8 * G * width * width * depth,
            bytes_accessed=2 * wide_count * samples * (cells + BX),
            transcendentals=0,
        ),
    )(offsets, band, jnp.asarray(line_table), jnp.asarray(row_table), x_weight[0], cross_weight[0])
    return out[None]


def solution(mesh):
    return jax.shard_map(
        per_device,
        mesh=mesh,
        in_specs=(
            P(None, "wide", "narrow", None),
            P(),
            P(("wide", "narrow"), None),
            P(("wide", "narrow"), None, None, None),
            P(("wide", "narrow"), None, None, None),
        ),
        out_specs=P(("wide", "narrow"), None, None, None),
        check_vma=False,
    )
```
